32 devices in a mesh: member: 2 (over x), node: 16 (over z, y, core).
Axes of the slice: x: 2, y: 2, z: 4, core: 2. Of those that a mesh axis runs over, the one named last changes fastest.
Arguments:
- latent: bfloat16 [4, 4096, 512], P('member', 'node'), may hold values from -6 to 6
- noise_draw: float32 [4, 32], P('member'), may hold values from -4 to 4
- mesh_links: int32 [6, 4096], P(None, 'node'), may hold values from 0 to 4095, as said below
- w_cond: float32 [2, 32, 512], replicated, may hold values from -0.3 to 0.3
- w_in: bfloat16 [2, 1024, 512], replicated, may hold values from -0.1875 to 0.1875
- w_out: bfloat16 [2, 512, 512], replicated, may hold values from -0.25 to 0.25
- dec_gain: float32 [512], replicated, may hold values from 0.5 to 1.5
- w_dec: bfloat16 [83, 512], replicated, may hold values from -2 to 2
- target_vertex_map: int32 [16384], P('node'), may hold values from 0 to 4095, as said below
- prior_field: bfloat16 [83, 16384], P(None, 'node'), may hold values from -6 to 6
- target: bfloat16 [83, 16384], P(None, 'node'), may hold values from -6 to 6
- location_loss_factor: float32 [16384], P('node'), may hold values from 8 to 24
Outputs:
- prediction_sensitivity: bfloat16 [4, 83, 16384], P('member', None, 'node')
- vertex_attribute_sensitivity: bfloat16 [4, 4096, 512], P('member', 'node')
The draws below stay inside these ranges and needn't reach their ends.
Inputs may be any that keep to these rules, and one draw needn't show every extreme that they name: mesh_links[k, n] = (n + s) mod 4096 with 1 <= |s| <= 96: every neighbour of a node lies within 96 positions of it along the node order, counted around the end. target_vertex_map[g] // 256 == g // 1024.
All inputs are finite; a program needn't handle non-finite values.
Results may differ from the reference program's by a relative error of at most 0.007.
Values may be sent and summed in bfloat16 or wider, within the bound.
A program may use at most 64 MiB of HBM per device.

```python
import math
import jax
import jax.numpy as jnp
from jax import lax

LAT = 512
CH = 83
NOISE = 32
LAYERS = 2
LINKS = 6
WIN = 96
NODE_DEV = 256
GRID_DEV = 1024
MEMBERS = 4
NODES = 4096
GRID = 16384


def draw_mesh_links(key, part):
    magnitude = jax.random.randint(jax.random.fold_in(key, 11), (LINKS, NODES), 1, WIN + 1)
    direction = jax.random.randint(jax.random.fold_in(key, 12), (LINKS, NODES), 0, 2) * 2 - 1
    positions = jnp.arange(NODES, dtype=jnp.int32)[None, :]
    return jnp.mod(positions + magnitude * direction, NODES).astype(jnp.int32)


def draw_target_vertex_map(key, part):
    local_node = jax.random.randint(jax.random.fold_in(key, 21), (GRID,), 0, NODE_DEV)
    shard_index = jnp.arange(GRID, dtype=jnp.int32) // GRID_DEV
    return (shard_index * NODE_DEV + local_node).astype(jnp.int32)


def draw_w_dec(key, part):
    levels = jax.random.uniform(jax.random.fold_in(key, 31), (CH, 1), jnp.float32, 0.0, jnp.log(32.0))
    row_scale = jnp.exp(levels)
    row_scale = row_scale / jnp.sqrt(jnp.mean(row_scale * row_scale))
    entries = jax.random.normal(jax.random.fold_in(key, 33), (CH, LAT), jnp.float32) * row_scale / jnp.sqrt(jnp.float32(LAT))
    return jnp.clip(entries, -2.0, 2.0).astype(jnp.bfloat16)


def shard_levels(key, dims, shards, low, high):
    factor_of, own = 1.0, jax.random.fold_in(key, 6)
    for position, parts in shards:
        heights = jnp.exp(jax.random.uniform(jax.random.fold_in(own, position), (parts,), jnp.float32, low / len(shards), high / len(shards)))
        factor_of = factor_of * jnp.repeat(heights, dims[position] // parts).reshape([-1 if axis == position else 1 for axis in range(len(dims))])
    return factor_of


def normal_values(stream_key, dims, deviation, reach, pieces=(), kind=jnp.bfloat16):
    gain = shard_levels(stream_key, dims, pieces, -0.22, 0.18) if pieces else 1.0
    array = jax.random.normal(stream_key, dims, jnp.float32) * deviation * gain
    return jnp.minimum(jnp.maximum(array, -reach), reach).astype(kind)


def setup_inputs(seed: int = 0) -> dict:
    seeds = jax.random.split(jax.random.key(seed), 13)
    latent = normal_values(seeds[0], (MEMBERS, NODES, LAT), 1.0, 6.0, ((0, 2), (1, 16)))
    noise_draw = normal_values(seeds[1], (MEMBERS, NOISE), 1.0, 4.0, ((0, 2),), jnp.float32)
    mesh_links = draw_mesh_links(jax.random.fold_in(seeds[12], 71), 0)
    w_cond = normal_values(seeds[3], (LAYERS, NOISE, LAT), 0.05, 0.3, (), jnp.float32)
    w_in = normal_values(seeds[4], (LAYERS, 2 * LAT, LAT), (2 * LAT) ** -0.5, 0.1875)
    w_out = normal_values(seeds[5], (LAYERS, LAT, LAT), LAT ** -0.5, 0.25)
    dec_gain = jnp.clip(1.0 + 0.1 * jax.random.normal(seeds[6], (LAT,), jnp.float32), 0.5, 1.5)
    w_dec = draw_w_dec(jax.random.fold_in(seeds[12], 71), 0)
    target_vertex_map = draw_target_vertex_map(jax.random.fold_in(seeds[12], 71), 0)
    prior_field = normal_values(seeds[9], (CH, GRID), 1.0, 6.0, ((1, 16),))
    target = normal_values(seeds[10], (CH, GRID), 1.0, 6.0, ((1, 16),))
    location_loss_factor = jnp.clip(jnp.exp(math.log(24.0) - 1.0986123 * jax.random.uniform(seeds[11], (GRID,), jnp.float32) ** shard_levels(seeds[11], (GRID,), ((0, 16),), -0.2, 0.2)), 8.0, 24.0)
    return dict(latent=latent, noise_draw=noise_draw, mesh_links=mesh_links, w_cond=w_cond, w_in=w_in, w_out=w_out, dec_gain=dec_gain, w_dec=w_dec, target_vertex_map=target_vertex_map, prior_field=prior_field, target=target, location_loss_factor=location_loss_factor)


NORM_EPS = 1e-06
DIST_EPS = 1e-06

def apply_layer_norm(values, scaling):
    inverse = lax.rsqrt(lax.optimization_barrier(jnp.mean(values * values, axis=-1, keepdims=True)) + NORM_EPS)
    return (values * inverse * scaling).astype(jnp.bfloat16)

def member_features(latent_row, noise_row, mesh_links, w_cond, w_in, w_out, dec_gain):
    processor_state = latent_row.astype(jnp.float32)
    for current_layer_index in range(LAYERS):
        scaling = 1.0 + jnp.dot(noise_row, w_cond[current_layer_index], precision=lax.Precision.HIGHEST)
        normalized_rows = apply_layer_norm(processor_state, scaling)
        summed = jnp.zeros(processor_state.shape, jnp.float32)
        for slot_index in range(LINKS):
            summed = summed + jnp.take(normalized_rows, mesh_links[slot_index], axis=0).astype(jnp.float32)
        neighbours = (summed / LINKS).astype(jnp.bfloat16)
        joined = jnp.concatenate([normalized_rows, neighbours], axis=1)
        preact = jnp.dot(joined, w_in[current_layer_index], preferred_element_type=jnp.float32)
        activated = jax.nn.silu(preact).astype(jnp.bfloat16)
        processor_state = processor_state + jnp.dot(activated, w_out[current_layer_index], preferred_element_type=jnp.float32)
    return apply_layer_norm(processor_state, dec_gain)

def reference(latent, noise_draw, mesh_links, w_cond, w_in, w_out, dec_gain, w_dec, target_vertex_map, prior_field, target, location_loss_factor):

    def per_member(operands):
        latent_row, noise_row = operands
        features = member_features(latent_row, noise_row, mesh_links, w_cond, w_in, w_out, dec_gain)
        return jnp.dot(w_dec, features.T, preferred_element_type=jnp.float32)
    readout_result = lax.map(per_member, (latent, noise_draw))
    ensemble_prediction = (prior_field.astype(jnp.float32)[None] + jnp.take(readout_result, target_vertex_map, axis=2)).astype(jnp.bfloat16)
    ensemble_size = ensemble_prediction.astype(jnp.float32)
    truth_all = target.astype(jnp.float32)

    def add_pull(carried, other_member):
        offset = ensemble_size - other_member[None]
        spread = jnp.sqrt(lax.optimization_barrier(jnp.sum(offset * offset, axis=1, keepdims=True)) + DIST_EPS)
        return (carried + offset / spread, None)
    pull_sums = lax.scan(add_pull, jnp.zeros_like(ensemble_size), ensemble_size)[0]
    missed = ensemble_size - truth_all[None]
    reached = jnp.sqrt(lax.optimization_barrier(jnp.sum(missed * missed, axis=1, keepdims=True)) + DIST_EPS)
    ensemble = MEMBERS
    skill_measures = missed / (ensemble * reached) - pull_sums / (ensemble * (ensemble - 1))
    prediction_sensitivity = (location_loss_factor[None, None, :] * skill_measures).astype(jnp.bfloat16)

    def per_vertex_quantities(grad_row):
        return jax.ops.segment_sum(grad_row.astype(jnp.float32).T, target_vertex_map, num_segments=NODES)
    vertex_sensitivity = lax.map(per_vertex_quantities, prediction_sensitivity)
    vertex_attribute_sensitivity = jnp.einsum('mnc,cl->mnl', vertex_sensitivity, w_dec.astype(jnp.float32), precision=lax.Precision.HIGHEST).astype(jnp.bfloat16)
    return (prediction_sensitivity, vertex_attribute_sensitivity)
```

```python
import functools

import jax
import jax.numpy as jnp
from jax import lax
from jax.experimental import pallas as pl
from jax.experimental.pallas import tpu as pltpu
from jax.sharding import PartitionSpec as P

WIN = 96
NORM_EPS = 1e-06
DIST_EPS = 1e-06
PLANES = 2
LANES = 128
F32 = jnp.float32
BF16 = jnp.bfloat16

NT = (((1,), (1,)), ((), ()))


def dot(a, b):
    return jnp.dot(a, b, preferred_element_type=F32)


def norm(values, gain):
    inverse = lax.rsqrt(jnp.mean(values * values, axis=-1, keepdims=True) + NORM_EPS)
    return (values * inverse * gain).astype(BF16)


def kernel(
    groups,
    shards,
    latent,
    noise,
    links,
    w_cond,
    dec_gain,
    w_dec,
    vertex_map,
    weights,
    w_in,
    w_out,
    prior_hbm,
    target_hbm,
    sens,
    vas,
    wi,
    wo,
    prior,
    target,
    state,
    normed,
    halo,
    part,
    pre,
    count_own,
    count_halo,
    onehot,
    wdp,
    dec,
    dec_in,
    own,
    other,
    load_sem,
    hs_sem,
    hr_sem,
    ds_sem,
    dr_sem,
):
    members, rows, width = latent.shape
    layers = w_in.shape[0]
    slots = links.shape[0]
    channels = w_dec.shape[0]
    points = vertex_map.shape[1]
    padded = wdp.shape[0]
    me = lax.axis_index("node")
    mine = lax.axis_index("member")
    right = lax.rem(me + 1, shards)
    left = lax.rem(me + shards - 1, shards)
    peers = [lax.rem(mine + k, groups) for k in range(1, groups)]

    barrier = pltpu.get_barrier_semaphore()
    for node in (left, right):
        pl.semaphore_signal(barrier, inc=1, device_id={"node": node}, device_id_type=pl.DeviceIdType.MESH)
    for peer in peers:
        pl.semaphore_signal(barrier, inc=1, device_id={"member": peer}, device_id_type=pl.DeviceIdType.MESH)

    loads = []
    for l in range(layers):
        loads.append(pltpu.make_async_copy(w_in.at[l], wi.at[l], load_sem.at[2 * l]))
        loads.append(pltpu.make_async_copy(w_out.at[l], wo.at[l], load_sem.at[2 * l + 1]))
    loads.append(pltpu.make_async_copy(prior_hbm, prior, load_sem.at[2 * layers]))
    loads.append(pltpu.make_async_copy(target_hbm, target, load_sem.at[2 * layers + 1]))
    for load in loads:
        load.start()

    gains = [
        1.0
        + jnp.dot(
            noise[...],
            w_cond[l],
            precision=lax.Precision.HIGHEST,
            preferred_element_type=F32,
        )
        for l in range(layers)
    ]

    halo_copies = {}

    def send_halo(l, m):
        pair = [
            pltpu.make_async_remote_copy(
                src_ref=normed.at[l, m, pl.ds(rows - WIN, WIN)],
                dst_ref=halo.at[l, m, pl.ds(0, WIN)],
                send_sem=hs_sem.at[l, m, 0],
                recv_sem=hr_sem.at[l, m, 0],
                device_id={"node": right},
                device_id_type=pl.DeviceIdType.MESH,
            ),
            pltpu.make_async_remote_copy(
                src_ref=normed.at[l, m, pl.ds(0, WIN)],
                dst_ref=halo.at[l, m, pl.ds(WIN, WIN)],
                send_sem=hs_sem.at[l, m, 1],
                recv_sem=hr_sem.at[l, m, 1],
                device_id={"node": left},
                device_id_type=pl.DeviceIdType.MESH,
            ),
        ]
        for copy in pair:
            copy.start()
        halo_copies[l, m] = pair

    for m in range(members):
        values = latent[m].astype(F32)
        normed[0, m] = norm(values, gains[0][m : m + 1])
        state[m] = values
        if m == 0:
            pl.semaphore_wait(barrier, 2 + len(peers))
        send_halo(0, m)

    total = rows * shards
    place = lax.rem(links[...] - (me * rows - WIN) + total, total)
    ids = lax.broadcasted_iota(jnp.int32, (rows, rows), 0) + WIN
    counts = jnp.zeros((rows, rows), F32)
    for k in range(slots):
        counts = counts + jnp.where(ids == place[k : k + 1, :], 1.0, 0.0)
    count_own[...] = counts.T.astype(BF16)
    ids = lax.broadcasted_iota(jnp.int32, (2 * WIN, rows), 0)
    ids = jnp.where(ids < WIN, ids, ids + rows)
    counts = jnp.zeros((2 * WIN, rows), F32)
    for k in range(slots):
        counts = counts + jnp.where(ids == place[k : k + 1, :], 1.0, 0.0)
    count_halo[...] = counts.T.astype(BF16)

    def own_part(l, m):
        rows_bf = normed[l, m]
        part[m] = dot(count_own[...], rows_bf)
        pre[m] = dot(rows_bf, wi[l, 0:width])

    dec_copies = []
    for l in range(layers):
        loads[2 * l].wait()
        for m in range(members):
            own_part(l, m)
        if l == 0:
            local = vertex_map[...] - me * rows
            nodes = lax.broadcasted_iota(jnp.int32, (rows, points), 0)
            onehot[...] = jnp.where(nodes == local, 1.0, 0.0).astype(BF16)
            wdp[...] = jnp.zeros_like(wdp)
            wdp[0:channels] = w_dec[...]
        loads[2 * l + 1].wait()
        for m in range(members):
            for copy in halo_copies[l, m]:
                copy.wait_recv()
            summed = part[m] + dot(count_halo[...], halo[l, m])
            neighbours = (summed * (1.0 / slots)).astype(BF16)
            preact = pre[m] + dot(neighbours, wi[l, width : 2 * width])
            activated = (preact / (1.0 + jnp.exp(-preact))).astype(BF16)
            values = state[m] + dot(activated, wo[l])
            if l + 1 < layers:
                state[m] = values
                normed[l + 1, m] = norm(values, gains[l + 1][m : m + 1])
                send_halo(l + 1, m)
            else:
                features = norm(values, dec_gain[...])
                decoded = lax.dot_general(wdp[...], features, NT, preferred_element_type=F32)
                for plane in range(PLANES):
                    piece = decoded.astype(BF16)
                    dec[m, plane] = piece
                    if plane + 1 < PLANES:
                        decoded = decoded - piece.astype(F32)
                for k, peer in enumerate(peers):
                    copy = pltpu.make_async_remote_copy(
                        src_ref=dec.at[m],
                        dst_ref=dec_in.at[k, m],
                        send_sem=ds_sem.at[k, m],
                        recv_sem=dr_sem.at[k, m],
                        device_id={"member": peer},
                        device_id_type=pl.DeviceIdType.MESH,
                    )
                    copy.start()
                    dec_copies.append((k, m, copy))

    for load in loads[2 * layers :]:
        load.wait()

    def forecast(planes):
        gathered = dot(planes[0], onehot[...])
        for plane in range(1, PLANES):
            gathered = gathered + dot(planes[plane], onehot[...])
        return (gathered[0:channels] + prior[...].astype(F32)).astype(BF16)

    for m in range(members):
        own[m] = forecast([dec[m, plane] for plane in range(PLANES)])
    for k, m, copy in dec_copies:
        copy.wait_recv()
        other[k * members + m] = forecast([dec_in[k, m, plane] for plane in range(PLANES)])

    ensemble = members * groups

    def unit(offset):
        return offset * lax.rsqrt(jnp.sum(offset * offset, axis=0, keepdims=True) + DIST_EPS)

    def points_step(step, carry):
        cut = pl.ds(pl.multiple_of(step * LANES, LANES), LANES)
        anchors = [own[m, :, cut].astype(F32) for m in range(members)]
        pulls = [None] * members

        def add(m, value):
            pulls[m] = value if pulls[m] is None else pulls[m] + value

        for a in range(members):
            for b in range(a + 1, members):
                pull = unit(anchors[a] - anchors[b])
                add(a, pull)
                add(b, -pull)
        for b in range(other.shape[0]):
            values = other[b, :, cut].astype(F32)
            for a in range(members):
                add(a, unit(anchors[a] - values))
        truth = target[:, cut].astype(F32)
        weight = weights[:, cut]
        for a in range(members):
            skill = unit(anchors[a] - truth) * (1.0 / ensemble)
            if ensemble > 1:
                skill = skill - pulls[a] * (1.0 / (ensemble * (ensemble - 1)))
            sens[a, :, cut] = (weight * skill).astype(BF16)
        return carry

    lax.fori_loop(0, points // LANES, points_step, 0)

    for m in range(members):
        node_grad = lax.dot_general(onehot[...], sens[m], NT, preferred_element_type=F32)
        high = node_grad.astype(BF16)
        low = (node_grad - high.astype(F32)).astype(BF16)
        vas[m] = (dot(high, w_dec[...]) + dot(low, w_dec[...])).astype(BF16)

    for pair in halo_copies.values():
        for copy in pair:
            copy.wait_send()
    for _, _, copy in dec_copies:
        copy.wait_send()


def per_device(
    latent,
    noise_draw,
    mesh_links,
    w_cond,
    w_in,
    w_out,
    dec_gain,
    w_dec,
    target_vertex_map,
    prior_field,
    target,
    location_loss_factor,
):
    groups = lax.axis_size("member")
    shards = lax.axis_size("node")
    members, rows, width = latent.shape
    layers = w_in.shape[0]
    channels = w_dec.shape[0]
    points = target_vertex_map.shape[0]
    padded = -(-channels // 16) * 16
    vmem = pl.BlockSpec(memory_space=pltpu.VMEM)
    hbm = pl.BlockSpec(memory_space=pl.ANY)
    far = max(groups - 1, 1)
    return pl.pallas_call(
        functools.partial(kernel, groups, shards),
        out_shape=(
            jax.ShapeDtypeStruct((members, channels, points), BF16),
            jax.ShapeDtypeStruct((members, rows, width), BF16),
        ),
        in_specs=[vmem] * 8 + [hbm] * 4,
        out_specs=(vmem, vmem),
        scratch_shapes=[
            pltpu.VMEM(w_in.shape, BF16),
            pltpu.VMEM(w_out.shape, BF16),
            pltpu.VMEM((channels, points), BF16),
            pltpu.VMEM((channels, points), BF16),
            pltpu.VMEM((members, rows, width), F32),
            pltpu.VMEM((layers, members, rows, width), BF16),
            pltpu.VMEM((layers, members, 2 * WIN, width), BF16),
            pltpu.VMEM((members, rows, width), F32),
            pltpu.VMEM((members, rows, width), F32),
            pltpu.VMEM((rows, rows), BF16),
            pltpu.VMEM((rows, 2 * WIN), BF16),
            pltpu.VMEM((rows, points), BF16),
            pltpu.VMEM((padded, width), BF16),
            pltpu.VMEM((members, PLANES, padded, rows), BF16),
            pltpu.VMEM((far, members, PLANES, padded, rows), BF16),
            pltpu.VMEM((members, channels, points), BF16),
            pltpu.VMEM((far * members, channels, points), BF16),
            pltpu.SemaphoreType.DMA((2 * layers + 2,)),
            pltpu.SemaphoreType.DMA((layers, members, 2)),
            pltpu.SemaphoreType.DMA((layers, members, 2)),
            pltpu.SemaphoreType.DMA((far, members)),
            pltpu.SemaphoreType.DMA((far, members)),
        ],
        compiler_params=pltpu.CompilerParams(
            collective_id=0, has_side_effects=True, vmem_limit_bytes=62 * 1024 * 1024
        ),
    )(
        latent,
        noise_draw,
        mesh_links,
        w_cond,
        dec_gain.reshape(1, width),
        w_dec,
        target_vertex_map.reshape(1, points),
        location_loss_factor.reshape(1, points),
        w_in,
        w_out,
        prior_field,
        target,
    )


def solution(mesh):
    in_specs = (
        P("member", "node", None),
        P("member", None),
        P(None, "node"),
        P(),
        P(),
        P(),
        P(),
        P(),
        P("node"),
        P(None, "node"),
        P(None, "node"),
        P("node"),
    )
    out_specs = (P("member", None, "node"), P("member", "node", None))
    return jax.shard_map(
        per_device, mesh=mesh, in_specs=in_specs, out_specs=out_specs, check_vma=False
    )
```

```python
import functools

import jax
import jax.numpy as jnp
from jax import lax
from jax.experimental import pallas as pl
from jax.experimental.pallas import tpu as pltpu
from jax.sharding import PartitionSpec as P

WIN = 96
NORM_EPS = 1e-06
DIST_EPS = 1e-06
PLANES = 2
LANES = 128
F32 = jnp.float32
BF16 = jnp.bfloat16

NT = (((1,), (1,)), ((), ()))


def dot(a, b):
    return jnp.dot(a, b, preferred_element_type=F32)


def norm(values, gain):
    inverse = lax.rsqrt(jnp.mean(values * values, axis=-1, keepdims=True) + NORM_EPS)
    return (values * inverse * gain).astype(BF16)


def kernel(
    groups,
    shards,
    latent,
    noise,
    links,
    w_cond,
    dec_gain,
    w_dec,
    vertex_map,
    weights,
    w_in,
    w_out,
    prior_hbm,
    target_hbm,
    sens,
    vas,
    wi,
    wo,
    prior,
    target,
    state,
    normed,
    halo,
    part,
    pre,
    count_own,
    count_halo,
    onehot,
    wdp,
    dec,
    dec_in,
    own,
    other,
    skill,
    load_sem,
    hs_sem,
    hr_sem,
    ds_sem,
    dr_sem,
):
    members, rows, width = latent.shape
    layers = w_in.shape[0]
    slots = links.shape[0]
    channels = w_dec.shape[0]
    points = vertex_map.shape[1]
    me = lax.axis_index("node")
    mine = lax.axis_index("member")
    right = lax.rem(me + 1, shards)
    left = lax.rem(me + shards - 1, shards)
    peers = [lax.rem(mine + k, groups) for k in range(1, groups)]

    barrier = pltpu.get_barrier_semaphore()
    for node in (left, right):
        pl.semaphore_signal(barrier, inc=1, device_id={"node": node}, device_id_type=pl.DeviceIdType.MESH)
    for peer in peers:
        pl.semaphore_signal(barrier, inc=1, device_id={"member": peer}, device_id_type=pl.DeviceIdType.MESH)

    loads = []
    for l in range(layers):
        loads.append(pltpu.make_async_copy(w_in.at[l], wi.at[l], load_sem.at[2 * l]))
        loads.append(pltpu.make_async_copy(w_out.at[l], wo.at[l], load_sem.at[2 * l + 1]))
    loads.append(pltpu.make_async_copy(prior_hbm, prior, load_sem.at[2 * layers]))
    loads.append(pltpu.make_async_copy(target_hbm, target, load_sem.at[2 * layers + 1]))
    for load in loads:
        load.start()

    gains = [
        1.0
        + jnp.dot(
            noise[...],
            w_cond[l],
            precision=lax.Precision.HIGHEST,
            preferred_element_type=F32,
        )
        for l in range(layers)
    ]

    halo_copies = {}

    def send_halo(l, m):
        pair = [
            pltpu.make_async_remote_copy(
                src_ref=normed.at[l, m, pl.ds(rows - WIN, WIN)],
                dst_ref=halo.at[l, m, pl.ds(0, WIN)],
                send_sem=hs_sem.at[l, m, 0],
                recv_sem=hr_sem.at[l, m, 0],
                device_id={"node": right},
                device_id_type=pl.DeviceIdType.MESH,
            ),
            pltpu.make_async_remote_copy(
                src_ref=normed.at[l, m, pl.ds(0, WIN)],
                dst_ref=halo.at[l, m, pl.ds(WIN, WIN)],
                send_sem=hs_sem.at[l, m, 1],
                recv_sem=hr_sem.at[l, m, 1],
                device_id={"node": left},
                device_id_type=pl.DeviceIdType.MESH,
            ),
        ]
        for copy in pair:
            copy.start()
        halo_copies[l, m] = pair

    for m in range(members):
        values = latent[m].astype(F32)
        normed[0, m] = norm(values, gains[0][m : m + 1])
        state[m] = values
        if m == 0:
            pl.semaphore_wait(barrier, 2 + len(peers))
        send_halo(0, m)

    total = rows * shards
    place = lax.rem(links[...] - (me * rows - WIN) + total, total)
    ids = lax.broadcasted_iota(jnp.int32, (rows, rows), 0) + WIN
    counts = jnp.zeros((rows, rows), F32)
    for k in range(slots):
        counts = counts + jnp.where(ids == place[k : k + 1, :], 1.0, 0.0)
    count_own[...] = counts.T.astype(BF16)
    ids = lax.broadcasted_iota(jnp.int32, (2 * WIN, rows), 0)
    ids = jnp.where(ids < WIN, ids, ids + rows)
    counts = jnp.zeros((2 * WIN, rows), F32)
    for k in range(slots):
        counts = counts + jnp.where(ids == place[k : k + 1, :], 1.0, 0.0)
    count_halo[...] = counts.T.astype(BF16)

    def own_part(l, m):
        rows_bf = normed[l, m]
        part[m] = dot(count_own[...], rows_bf)
        pre[m] = dot(rows_bf, wi[l, 0:width])

    dec_copies = []
    for l in range(layers):
        loads[2 * l].wait()
        for m in range(members):
            own_part(l, m)
        if l == 0:
            local = vertex_map[...] - me * rows
            nodes = lax.broadcasted_iota(jnp.int32, (rows, points), 0)
            onehot[...] = jnp.where(nodes == local, 1.0, 0.0).astype(BF16)
            wdp[...] = jnp.zeros_like(wdp)
            wdp[0:channels] = w_dec[...]
        loads[2 * l + 1].wait()
        for m in range(members):
            for copy in halo_copies[l, m]:
                copy.wait_recv()
            summed = part[m] + dot(count_halo[...], halo[l, m])
            neighbours = (summed * (1.0 / slots)).astype(BF16)
            preact = pre[m] + dot(neighbours, wi[l, width : 2 * width])
            activated = (preact / (1.0 + jnp.exp(-preact))).astype(BF16)
            values = state[m] + dot(activated, wo[l])
            if l + 1 < layers:
                state[m] = values
                normed[l + 1, m] = norm(values, gains[l + 1][m : m + 1])
                send_halo(l + 1, m)
            else:
                features = norm(values, dec_gain[...])
                decoded = lax.dot_general(wdp[...], features, NT, preferred_element_type=F32)
                for plane in range(PLANES):
                    piece = decoded.astype(BF16)
                    dec[m, plane] = piece
                    if plane + 1 < PLANES:
                        decoded = decoded - piece.astype(F32)
                for k, peer in enumerate(peers):
                    copy = pltpu.make_async_remote_copy(
                        src_ref=dec.at[m],
                        dst_ref=dec_in.at[k, m],
                        send_sem=ds_sem.at[k, m],
                        recv_sem=dr_sem.at[k, m],
                        device_id={"member": peer},
                        device_id_type=pl.DeviceIdType.MESH,
                    )
                    copy.start()
                    dec_copies.append((k, m, copy))

    for load in loads[2 * layers :]:
        load.wait()

    def forecast(planes):
        gathered = dot(planes[0], onehot[...])
        for plane in range(1, PLANES):
            gathered = gathered + dot(planes[plane], onehot[...])
        return (gathered[0:channels] + prior[...].astype(F32)).astype(BF16)

    ensemble = members * groups
    skill_scale = 1.0 / ensemble
    pull_scale = 1.0 / (ensemble * max(ensemble - 1, 1))

    def unit(offset, scale):
        inverse = lax.rsqrt(jnp.sum(offset * offset, axis=0, keepdims=True) + DIST_EPS)
        return offset * (inverse * scale)

    def points_loop(body):
        def step(i, carry):
            body(pl.ds(pl.multiple_of(i * LANES, LANES), LANES))
            return carry

        lax.fori_loop(0, points // LANES, step, 0, unroll=2)

    for m in range(members):
        own[m] = forecast([dec[m, plane] for plane in range(PLANES)])

    def own_terms(cut):
        anchors = [own[m, :, cut].astype(F32) for m in range(members)]
        truth = target[:, cut].astype(F32)
        skills = [unit(anchor - truth, skill_scale) for anchor in anchors]
        for a in range(members):
            for b in range(a + 1, members):
                pull = unit(anchors[a] - anchors[b], pull_scale)
                skills[a] = skills[a] - pull
                skills[b] = skills[b] + pull
        for a in range(members):
            if dec_copies:
                skill[a, :, cut] = skills[a]
            else:
                sens[a, :, cut] = (weights[:, cut] * skills[a]).astype(BF16)

    points_loop(own_terms)

    for i, (k, m, copy) in enumerate(dec_copies):
        copy.wait_recv()
        other[...] = forecast([dec_in[k, m, plane] for plane in range(PLANES)])

        def other_terms(cut, last=i + 1 == len(dec_copies)):
            values = other[:, cut].astype(F32)
            for a in range(members):
                anchor = own[a, :, cut].astype(F32)
                total = skill[a, :, cut] - unit(anchor - values, pull_scale)
                if last:
                    sens[a, :, cut] = (weights[:, cut] * total).astype(BF16)
                else:
                    skill[a, :, cut] = total

        points_loop(other_terms)

    for m in range(members):
        node_grad = lax.dot_general(onehot[...], sens[m], NT, preferred_element_type=F32)
        high = node_grad.astype(BF16)
        low = (node_grad - high.astype(F32)).astype(BF16)
        vas[m] = (dot(high, w_dec[...]) + dot(low, w_dec[...])).astype(BF16)

    for pair in halo_copies.values():
        for copy in pair:
            copy.wait_send()
    for _, _, copy in dec_copies:
        copy.wait_send()


def per_device(
    latent,
    noise_draw,
    mesh_links,
    w_cond,
    w_in,
    w_out,
    dec_gain,
    w_dec,
    target_vertex_map,
    prior_field,
    target,
    location_loss_factor,
):
    groups = lax.axis_size("member")
    shards = lax.axis_size("node")
    members, rows, width = latent.shape
    layers = w_in.shape[0]
    channels = w_dec.shape[0]
    points = target_vertex_map.shape[0]
    padded = -(-channels // 16) * 16
    vmem = pl.BlockSpec(memory_space=pltpu.VMEM)
    hbm = pl.BlockSpec(memory_space=pltpu.HBM)
    far = max(groups - 1, 1)
    return pl.pallas_call(
        functools.partial(kernel, groups, shards),
        out_shape=(
            jax.ShapeDtypeStruct((members, channels, points), BF16),
            jax.ShapeDtypeStruct((members, rows, width), BF16),
        ),
        in_specs=[vmem] * 8 + [hbm] * 4,
        out_specs=(vmem, vmem),
        scratch_shapes=[
            pltpu.VMEM(w_in.shape, BF16),
            pltpu.VMEM(w_out.shape, BF16),
            pltpu.VMEM((channels, points), BF16),
            pltpu.VMEM((channels, points), BF16),
            pltpu.VMEM((members, rows, width), F32),
            pltpu.VMEM((layers, members, rows, width), BF16),
            pltpu.VMEM((layers, members, 2 * WIN, width), BF16),
            pltpu.VMEM((members, rows, width), F32),
            pltpu.VMEM((members, rows, width), F32),
            pltpu.VMEM((rows, rows), BF16),
            pltpu.VMEM((rows, 2 * WIN), BF16),
            pltpu.VMEM((rows, points), BF16),
            pltpu.VMEM((padded, width), BF16),
            pltpu.VMEM((members, PLANES, padded, rows), BF16),
            pltpu.VMEM((far, members, PLANES, padded, rows), BF16),
            pltpu.VMEM((members, channels, points), BF16),
            pltpu.VMEM((channels, points), BF16),
            pltpu.VMEM((members, channels, points), F32),
            pltpu.SemaphoreType.DMA((2 * layers + 2,)),
            pltpu.SemaphoreType.DMA((layers, members, 2)),
            pltpu.SemaphoreType.DMA((layers, members, 2)),
            pltpu.SemaphoreType.DMA((far, members)),
            pltpu.SemaphoreType.DMA((far, members)),
        ],
        compiler_params=pltpu.CompilerParams(
            collective_id=0, has_side_effects=True, vmem_limit_bytes=40 * 1024 * 1024
        ),
    )(
        pltpu.with_memory_space_constraint(latent, pltpu.HBM),
        pltpu.with_memory_space_constraint(noise_draw, pltpu.HBM),
        pltpu.with_memory_space_constraint(mesh_links, pltpu.HBM),
        pltpu.with_memory_space_constraint(w_cond, pltpu.HBM),
        pltpu.with_memory_space_constraint(dec_gain.reshape(1, width), pltpu.HBM),
        pltpu.with_memory_space_constraint(w_dec, pltpu.HBM),
        pltpu.with_memory_space_constraint(target_vertex_map.reshape(1, points), pltpu.HBM),
        pltpu.with_memory_space_constraint(location_loss_factor.reshape(1, points), pltpu.HBM),
        pltpu.with_memory_space_constraint(w_in, pltpu.HBM),
        pltpu.with_memory_space_constraint(w_out, pltpu.HBM),
        pltpu.with_memory_space_constraint(prior_field, pltpu.HBM),
        pltpu.with_memory_space_constraint(target, pltpu.HBM),
    )


def solution(mesh):
    in_specs = (
        P("member", "node", None),
        P("member", None),
        P(None, "node"),
        P(),
        P(),
        P(),
        P(),
        P(),
        P("node"),
        P(None, "node"),
        P(None, "node"),
        P("node"),
    )
    out_specs = (P("member", None, "node"), P("member", "node", None))
    return jax.shard_map(
        per_device, mesh=mesh, in_specs=in_specs, out_specs=out_specs, check_vma=False
    )
```

```python
import functools

import jax
import jax.numpy as jnp
from jax import lax
from jax.experimental import pallas as pl
from jax.experimental.pallas import tpu as pltpu
from jax.sharding import PartitionSpec as P

WIN = 96
NORM_EPS = 1e-06
DIST_EPS = 1e-06
PLANES = 2
LANES = 128
F32 = jnp.float32
BF16 = jnp.bfloat16

NT = (((1,), (1,)), ((), ()))


def dot(a, b):
    return jnp.dot(a, b, preferred_element_type=F32)


def norm(values, gain):
    inverse = lax.rsqrt(jnp.mean(values * values, axis=-1, keepdims=True) + NORM_EPS)
    return (values * inverse * gain).astype(BF16)


def kernel(
    groups,
    shards,
    latent,
    noise,
    links,
    w_cond,
    dec_gain,
    w_dec,
    vertex_map,
    weights,
    w_in,
    w_out,
    prior_hbm,
    target_hbm,
    sens,
    vas,
    wi,
    wo,
    prior,
    target,
    state,
    normed,
    halo,
    part,
    pre,
    count_own,
    count_halo,
    onehot,
    wdp,
    dec,
    dec_in,
    own,
    other,
    skill,
    load_sem,
    hs_sem,
    hr_sem,
    ds_sem,
    dr_sem,
):
    members, rows, width = latent.shape
    layers = w_in.shape[0]
    slots = links.shape[0]
    channels = w_dec.shape[0]
    points = vertex_map.shape[1]
    me = lax.axis_index("node")
    mine = lax.axis_index("member")
    right = lax.rem(me + 1, shards)
    left = lax.rem(me + shards - 1, shards)
    peers = [lax.rem(mine + k, groups) for k in range(1, groups)]

    barrier = pltpu.get_barrier_semaphore()
    for node in (left, right):
        pl.semaphore_signal(barrier, inc=1, device_id={"node": node}, device_id_type=pl.DeviceIdType.MESH)
    for peer in peers:
        pl.semaphore_signal(barrier, inc=1, device_id={"member": peer}, device_id_type=pl.DeviceIdType.MESH)

    loads = []
    for l in range(layers):
        loads.append(pltpu.make_async_copy(w_in.at[l], wi.at[l], load_sem.at[2 * l]))
        loads.append(pltpu.make_async_copy(w_out.at[l], wo.at[l], load_sem.at[2 * l + 1]))
    loads.append(pltpu.make_async_copy(prior_hbm, prior, load_sem.at[2 * layers]))
    loads.append(pltpu.make_async_copy(target_hbm, target, load_sem.at[2 * layers + 1]))
    for load in loads:
        load.start()

    def gain_of(l):
        return 1.0 + jnp.dot(
            noise[...],
            w_cond[l],
            precision=lax.Precision.HIGHEST,
            preferred_element_type=F32,
        )

    gains = [gain_of(0)]

    halo_copies = {}

    def send_halo(l, m):
        pair = [
            pltpu.make_async_remote_copy(
                src_ref=normed.at[l, m, pl.ds(rows - WIN, WIN)],
                dst_ref=halo.at[l, m, pl.ds(0, WIN)],
                send_sem=hs_sem.at[l, m, 0],
                recv_sem=hr_sem.at[l, m, 0],
                device_id={"node": right},
                device_id_type=pl.DeviceIdType.MESH,
            ),
            pltpu.make_async_remote_copy(
                src_ref=normed.at[l, m, pl.ds(0, WIN)],
                dst_ref=halo.at[l, m, pl.ds(WIN, WIN)],
                send_sem=hs_sem.at[l, m, 1],
                recv_sem=hr_sem.at[l, m, 1],
                device_id={"node": left},
                device_id_type=pl.DeviceIdType.MESH,
            ),
        ]
        for copy in pair:
            copy.start()
        halo_copies[l, m] = pair

    for m in range(members):
        values = latent[m].astype(F32)
        normed[0, m] = norm(values, gains[0][m : m + 1])
        state[m] = values
        if m == 0:
            pl.semaphore_wait(barrier, 2 + len(peers))
        send_halo(0, m)
    gains += [gain_of(l) for l in range(1, layers)]

    total = rows * shards
    place = lax.rem(links[...] - (me * rows - WIN) + total, total)
    ids = lax.broadcasted_iota(jnp.int32, (rows, rows), 0) + WIN
    counts = jnp.zeros((rows, rows), F32)
    for k in range(slots):
        counts = counts + jnp.where(ids == place[k : k + 1, :], 1.0, 0.0)
    count_own[...] = counts.T.astype(BF16)
    ids = lax.broadcasted_iota(jnp.int32, (2 * WIN, rows), 0)
    ids = jnp.where(ids < WIN, ids, ids + rows)
    counts = jnp.zeros((2 * WIN, rows), F32)
    for k in range(slots):
        counts = counts + jnp.where(ids == place[k : k + 1, :], 1.0, 0.0)
    count_halo[...] = counts.T.astype(BF16)

    def own_part(l, m):
        rows_bf = normed[l, m]
        part[m] = dot(count_own[...], rows_bf)
        pre[m] = dot(rows_bf, wi[l, 0:width])

    def forecast(planes):
        gathered = dot(planes[0], onehot[...])
        for plane in range(1, PLANES):
            gathered = gathered + dot(planes[plane], onehot[...])
        return (gathered[0:channels] + prior[...].astype(F32)).astype(BF16)

    dec_copies = []
    loads[0].wait()
    for m in range(members):
        own_part(0, m)
    for l in range(layers):
        if l == 0:
            local = vertex_map[...] - me * rows
            nodes = lax.broadcasted_iota(jnp.int32, (rows, points), 0)
            onehot[...] = jnp.where(nodes == local, 1.0, 0.0).astype(BF16)
            wdp[...] = jnp.zeros_like(wdp)
            wdp[0:channels] = w_dec[...]
        loads[2 * l + 1].wait()
        loads[2 * l + 2].wait()
        for m in range(members):
            for copy in halo_copies[l, m]:
                copy.wait_recv()
            summed = part[m] + dot(count_halo[...], halo[l, m])
            neighbours = (summed * (1.0 / slots)).astype(BF16)
            preact = pre[m] + dot(neighbours, wi[l, width : 2 * width])
            activated = (preact / (1.0 + jnp.exp(-preact))).astype(BF16)
            values = state[m] + dot(activated, wo[l])
            if l + 1 < layers:
                state[m] = values
                normed[l + 1, m] = norm(values, gains[l + 1][m : m + 1])
                send_halo(l + 1, m)
                own_part(l + 1, m)
            else:
                features = norm(values, dec_gain[...])
                decoded = lax.dot_general(wdp[...], features, NT, preferred_element_type=F32)
                for plane in range(PLANES):
                    piece = decoded.astype(BF16)
                    dec[m, plane] = piece
                    if plane + 1 < PLANES:
                        decoded = decoded - piece.astype(F32)
                for k, peer in enumerate(peers):
                    copy = pltpu.make_async_remote_copy(
                        src_ref=dec.at[m],
                        dst_ref=dec_in.at[k, m],
                        send_sem=ds_sem.at[k, m],
                        recv_sem=dr_sem.at[k, m],
                        device_id={"member": peer},
                        device_id_type=pl.DeviceIdType.MESH,
                    )
                    copy.start()
                    dec_copies.append((k, m, copy))
                own[m] = forecast([dec[m, plane] for plane in range(PLANES)])

    loads[2 * layers + 1].wait()

    ensemble = members * groups
    skill_scale = 1.0 / ensemble
    pull_scale = 1.0 / (ensemble * max(ensemble - 1, 1))

    def unit(offset, scale):
        inverse = lax.rsqrt(jnp.sum(offset * offset, axis=0, keepdims=True) + DIST_EPS)
        return offset * (inverse * scale)

    def points_loop(body):
        def step(i, carry):
            body(pl.ds(pl.multiple_of(i * LANES, LANES), LANES))
            return carry

        lax.fori_loop(0, points // LANES, step, 0, unroll=2)

    def own_terms(cut):
        anchors = [own[m, :, cut].astype(F32) for m in range(members)]
        truth = target[:, cut].astype(F32)
        skills = [unit(anchor - truth, skill_scale) for anchor in anchors]
        for a in range(members):
            for b in range(a + 1, members):
                pull = unit(anchors[a] - anchors[b], pull_scale)
                skills[a] = skills[a] - pull
                skills[b] = skills[b] + pull
        for a in range(members):
            if dec_copies:
                skill[a, :, cut] = skills[a]
            else:
                sens[a, :, cut] = (weights[:, cut] * skills[a]).astype(BF16)

    points_loop(own_terms)

    for i, (k, m, copy) in enumerate(dec_copies):
        copy.wait_recv()
        other[...] = forecast([dec_in[k, m, plane] for plane in range(PLANES)])

        def other_terms(cut, last=i + 1 == len(dec_copies)):
            values = other[:, cut].astype(F32)
            for a in range(members):
                anchor = own[a, :, cut].astype(F32)
                total = skill[a, :, cut] - unit(anchor - values, pull_scale)
                if last:
                    sens[a, :, cut] = (weights[:, cut] * total).astype(BF16)
                else:
                    skill[a, :, cut] = total

        points_loop(other_terms)

    for m in range(members):
        node_grad = lax.dot_general(onehot[...], sens[m], NT, preferred_element_type=F32)
        high = node_grad.astype(BF16)
        low = (node_grad - high.astype(F32)).astype(BF16)
        vas[m] = (dot(high, w_dec[...]) + dot(low, w_dec[...])).astype(BF16)

    for pair in halo_copies.values():
        for copy in pair:
            copy.wait_send()
    for _, _, copy in dec_copies:
        copy.wait_send()


def per_device(
    latent,
    noise_draw,
    mesh_links,
    w_cond,
    w_in,
    w_out,
    dec_gain,
    w_dec,
    target_vertex_map,
    prior_field,
    target,
    location_loss_factor,
):
    groups = lax.axis_size("member")
    shards = lax.axis_size("node")
    members, rows, width = latent.shape
    layers = w_in.shape[0]
    channels = w_dec.shape[0]
    points = target_vertex_map.shape[0]
    padded = -(-channels // 16) * 16
    vmem = pl.BlockSpec(memory_space=pltpu.VMEM)
    hbm = pl.BlockSpec(memory_space=pltpu.HBM)
    far = max(groups - 1, 1)
    return pl.pallas_call(
        functools.partial(kernel, groups, shards),
        out_shape=(
            jax.ShapeDtypeStruct((members, channels, points), BF16),
            jax.ShapeDtypeStruct((members, rows, width), BF16),
        ),
        in_specs=[vmem] * 8 + [hbm] * 4,
        out_specs=(vmem, vmem),
        scratch_shapes=[
            pltpu.VMEM(w_in.shape, BF16),
            pltpu.VMEM(w_out.shape, BF16),
            pltpu.VMEM((channels, points), BF16),
            pltpu.VMEM((channels, points), BF16),
            pltpu.VMEM((members, rows, width), F32),
            pltpu.VMEM((layers, members, rows, width), BF16),
            pltpu.VMEM((layers, members, 2 * WIN, width), BF16),
            pltpu.VMEM((members, rows, width), F32),
            pltpu.VMEM((members, rows, width), F32),
            pltpu.VMEM((rows, rows), BF16),
            pltpu.VMEM((rows, 2 * WIN), BF16),
            pltpu.VMEM((rows, points), BF16),
            pltpu.VMEM((padded, width), BF16),
            pltpu.VMEM((members, PLANES, padded, rows), BF16),
            pltpu.VMEM((far, members, PLANES, padded, rows), BF16),
            pltpu.VMEM((members, channels, points), BF16),
            pltpu.VMEM((channels, points), BF16),
            pltpu.VMEM((members, channels, points), F32),
            pltpu.SemaphoreType.DMA((2 * layers + 2,)),
            pltpu.SemaphoreType.DMA((layers, members, 2)),
            pltpu.SemaphoreType.DMA((layers, members, 2)),
            pltpu.SemaphoreType.DMA((far, members)),
            pltpu.SemaphoreType.DMA((far, members)),
        ],
        compiler_params=pltpu.CompilerParams(
            collective_id=0, has_side_effects=True, vmem_limit_bytes=40 * 1024 * 1024
        ),
    )(
        pltpu.with_memory_space_constraint(latent, pltpu.HBM),
        pltpu.with_memory_space_constraint(noise_draw, pltpu.HBM),
        pltpu.with_memory_space_constraint(mesh_links, pltpu.HBM),
        pltpu.with_memory_space_constraint(w_cond, pltpu.HBM),
        pltpu.with_memory_space_constraint(dec_gain.reshape(1, width), pltpu.HBM),
        pltpu.with_memory_space_constraint(w_dec, pltpu.HBM),
        pltpu.with_memory_space_constraint(target_vertex_map.reshape(1, points), pltpu.HBM),
        pltpu.with_memory_space_constraint(location_loss_factor.reshape(1, points), pltpu.HBM),
        pltpu.with_memory_space_constraint(w_in, pltpu.HBM),
        pltpu.with_memory_space_constraint(w_out, pltpu.HBM),
        pltpu.with_memory_space_constraint(prior_field, pltpu.HBM),
        pltpu.with_memory_space_constraint(target, pltpu.HBM),
    )


def solution(mesh):
    in_specs = (
        P("member", "node", None),
        P("member", None),
        P(None, "node"),
        P(),
        P(),
        P(),
        P(),
        P(),
        P("node"),
        P(None, "node"),
        P(None, "node"),
        P("node"),
    )
    out_specs = (P("member", None, "node"), P("member", "node", None))
    return jax.shard_map(
        per_device, mesh=mesh, in_specs=in_specs, out_specs=out_specs, check_vma=False
    )
```
